64 devices in a mesh: dp: 4 (over x, y), ep: 16 (over z, core).
Axes of the slice: x: 2, y: 2, z: 8, core: 2. Of those that a mesh axis runs over, the one named last changes fastest.
The devices are a block of a 4x4x8 slice.
Arguments:
- tokens: bfloat16 [16384, 2048], P(('dp', 'ep')), parts along dimension 0
- expert_ids: int32 [16384, 6], P(('dp', 'ep')), parts along dimension 0
- gate_vals: float32 [16384, 6], P(('dp', 'ep')), parts along dimension 0
- slots: int32 [16384, 6], P(('dp', 'ep')), parts along dimension 0
- shared_w1: bfloat16 [2048, 2816], replicated
- shared_w3: bfloat16 [2048, 2816], replicated
- shared_w2: bfloat16 [2816, 2048], replicated
- shared_gate: bfloat16 [2048], replicated
- expert_w1: bfloat16 [64, 2048, 1408], P('ep')
- expert_w3: bfloat16 [64, 2048, 1408], P('ep')
- expert_w2: bfloat16 [64, 1408, 2048], P('ep')
Outputs:
- output: bfloat16 [16384, 2048], P(('dp', 'ep')), parts along dimension 0
There are 4 independent parts. The reference program is written for one: setup_inputs(seed, part) draws one part's arguments, and reference() takes and returns one part's arrays. A program takes and returns all parts, laid end to end along the dimension named above; an argument that names none is the same for every part.
All inputs are finite; a program needn't handle non-finite values.
Results may differ from the reference program's by a relative error of at most 0.00517458.
Values are sent between devices in bfloat16 or wider.
A program may use at most 768 MiB of HBM per device.

```python
import jax
import jax.numpy as jnp
from jax import lax

EP_SIZE = 16
TOKENS_DEV = 256
HIDDEN = 2048
EXPERTS = 64
TOP_K = 6
EXPERT_FF = 1408
SHARED_FF = 2816
CAPACITY = 48

NUM_TOKENS = EP_SIZE * TOKENS_DEV
BUF_ROWS = EXPERTS * CAPACITY


def draw_routes(route_key):
    score_key, bias_key, hot_key = jax.random.split(route_key, 3)
    scores = jax.random.randint(score_key, (NUM_TOKENS, EXPERTS), 0, 4096)
    expert_bias = jax.random.randint(bias_key, (EXPERTS,), 0, 1024)
    hot_expert = jax.random.randint(hot_key, (), 0, EXPERTS)
    expert_pos = jnp.arange(EXPERTS)
    forced = ((jnp.arange(NUM_TOKENS) % 2) == 0)[:, None] & (expert_pos[None, :] == hot_expert)
    total_score = scores + expert_bias[None, :] + jnp.where(forced, 8192, 0)
    distinct = total_score * EXPERTS + expert_pos[None, :]
    return lax.top_k(distinct, TOP_K)[1].astype(jnp.int32)


def source_slots(src_ids):
    flat_ids = src_ids.reshape(TOKENS_DEV * TOP_K)
    one_hot = (flat_ids[:, None] == jnp.arange(EXPERTS)[None, :]).astype(jnp.int32)
    earlier = jnp.cumsum(one_hot, axis=0) - one_hot
    position = jnp.sum(earlier * one_hot, axis=1)
    return jnp.where(position < CAPACITY, position, -1).reshape(TOKENS_DEV, TOP_K).astype(jnp.int32)


def normal_stack(stack_key, rows, cols):
    def one_matrix(one_key):
        return (jax.random.normal(one_key, (rows, cols), jnp.float32) * rows ** -0.5).astype(jnp.bfloat16)
    return lax.map(one_matrix, jax.random.split(stack_key, EXPERTS))


def setup_inputs(seed: int = 0, part: int = 0) -> dict:
    part_key = jax.random.fold_in(jax.random.key(seed), part)
    tok_key, route_key, gate_key = jax.random.split(part_key, 3)
    weight_keys = jax.random.split(jax.random.key(seed + 1), 7)
    tokens = jax.random.normal(tok_key, (NUM_TOKENS, HIDDEN), jnp.float32).astype(jnp.bfloat16)
    expert_ids = draw_routes(route_key)
    slots = lax.map(source_slots, expert_ids.reshape(EP_SIZE, TOKENS_DEV, TOP_K)).reshape(NUM_TOKENS, TOP_K)
    gate_vals = jax.random.uniform(gate_key, (NUM_TOKENS, TOP_K), jnp.float32, 0.5, 1.5) * TOP_K ** -0.5
    shared_w1 = (jax.random.normal(weight_keys[0], (HIDDEN, SHARED_FF), jnp.float32) * HIDDEN ** -0.5).astype(jnp.bfloat16)
    shared_w3 = (jax.random.normal(weight_keys[1], (HIDDEN, SHARED_FF), jnp.float32) * HIDDEN ** -0.5).astype(jnp.bfloat16)
    shared_w2 = (jax.random.normal(weight_keys[2], (SHARED_FF, HIDDEN), jnp.float32) * SHARED_FF ** -0.5).astype(jnp.bfloat16)
    shared_gate = (jax.random.normal(weight_keys[3], (HIDDEN,), jnp.float32) * 2.0 * HIDDEN ** -0.5).astype(jnp.bfloat16)
    expert_w1 = normal_stack(weight_keys[4], HIDDEN, EXPERT_FF)
    expert_w3 = normal_stack(weight_keys[5], HIDDEN, EXPERT_FF)
    expert_w2 = normal_stack(weight_keys[6], EXPERT_FF, HIDDEN)
    return {'tokens': tokens, 'expert_ids': expert_ids, 'gate_vals': gate_vals, 'slots': slots, 'shared_w1': shared_w1, 'shared_w3': shared_w3, 'shared_w2': shared_w2, 'shared_gate': shared_gate, 'expert_w1': expert_w1, 'expert_w3': expert_w3, 'expert_w2': expert_w2}


def swiglu_rows(rows, w_up, w_in, w_down):
    act_a = jnp.dot(rows, w_up, preferred_element_type=jnp.float32)
    act_b = jnp.dot(rows, w_in, preferred_element_type=jnp.float32)
    hidden_act = (jax.nn.silu(act_a) * act_b).astype(jnp.bfloat16)
    return jnp.dot(hidden_act, w_down, preferred_element_type=jnp.float32)


def reference(tokens, expert_ids, gate_vals, slots, shared_w1, shared_w3, shared_w2, shared_gate, expert_w1, expert_w3, expert_w2):
    src_tokens = tokens.reshape(EP_SIZE, TOKENS_DEV, HIDDEN)
    kept_mask = slots >= 0
    slot_dest = jnp.where(kept_mask, expert_ids * CAPACITY + slots, BUF_ROWS)
    flat_dest = slot_dest.reshape(EP_SIZE, TOKENS_DEV * TOP_K)
    copy_tok = jnp.arange(TOKENS_DEV * TOP_K, dtype=jnp.int32) // TOP_K

    def dispatch_one(operands):
        src_rows, src_dest = operands
        row_owner = jnp.full((BUF_ROWS + 1,), TOKENS_DEV, jnp.int32).at[src_dest].set(copy_tok)
        return jnp.take(src_rows, row_owner[:BUF_ROWS], axis=0, mode='fill', fill_value=0)

    buffers = lax.map(dispatch_one, (src_tokens, flat_dest))
    per_expert = buffers.reshape(EP_SIZE, EXPERTS, CAPACITY, HIDDEN).transpose(1, 0, 2, 3).reshape(EXPERTS, EP_SIZE * CAPACITY, HIDDEN)

    def expert_one(operands):
        rows, w_up, w_in, w_down = operands
        return swiglu_rows(rows, w_up, w_in, w_down).astype(jnp.bfloat16)

    expert_out = lax.map(expert_one, (per_expert, expert_w1, expert_w3, expert_w2))
    returned = expert_out.reshape(EXPERTS, EP_SIZE, CAPACITY, HIDDEN).transpose(1, 0, 2, 3).reshape(EP_SIZE, BUF_ROWS, HIDDEN)
    weights = jnp.where(kept_mask, gate_vals, 0.0).reshape(EP_SIZE, TOKENS_DEV, TOP_K)
    src_dest = slot_dest.reshape(EP_SIZE, TOKENS_DEV, TOP_K)

    def combine_one(operands):
        src_rows, src_out, src_idx, src_weights = operands
        picked = jnp.take(src_out, src_idx, axis=0, mode='fill', fill_value=0)
        routed = jnp.einsum('tk,tkd->td', src_weights, picked.astype(jnp.float32))
        gate_logit = jnp.dot(src_rows, shared_gate, preferred_element_type=jnp.float32)
        shared_out = jax.nn.sigmoid(gate_logit)[:, None] * swiglu_rows(src_rows, shared_w1, shared_w3, shared_w2)
        return (src_rows.astype(jnp.float32) + shared_out + routed).astype(jnp.bfloat16)

    result = lax.map(combine_one, (src_tokens, returned, src_dest, weights))
    return result.reshape(NUM_TOKENS, HIDDEN)
```

```python
import jax
import jax.numpy as jnp
from jax import lax
from jax.sharding import PartitionSpec as P


def solution(mesh):
    num_ep = mesh.shape['ep']
    nz = num_ep // 2
    half = nz // 2
    row_spec = P(('dp', 'ep'), None)
    replicated = P()
    expert_spec = P('ep', None, None)
    plus = [(i, (i + 2) % num_ep) for i in range(num_ep)]
    minus = [(i, (i - 2) % num_ep) for i in range(num_ep)]
    swap = [(i, i ^ 1) for i in range(num_ep)]

    def send(x, perm):
        return lax.ppermute(x, 'ep', perm)

    def after(x, dep):
        return lax.optimization_barrier((x, dep))[0]

    def device_step(tokens, expert_ids, gate_vals, slots, shared_w1, shared_w3, shared_w2, shared_gate, expert_w1, expert_w3, expert_w2):
        tok_count, hidden = tokens.shape
        top_k = expert_ids.shape[1]
        local_experts = expert_w1.shape[0]
        num_experts = local_experts * num_ep
        capacity = 8 * ((2 * tok_count * top_k + 8 * num_experts - 1) // (8 * num_experts))
        core_rows = local_experts * capacity
        chip_rows = 2 * core_rows
        ep = lax.axis_index('ep')
        z, core = ep // 2, ep % 2
        half_tok = tok_count // 2

        code = jnp.where(slots >= 0, expert_ids * capacity + slots, -1).astype(jnp.float32)
        meta = jnp.concatenate([code.T, gate_vals.T, jnp.zeros((16 - 2 * top_k, tok_count), jnp.float32)], axis=0)

        fwd_tok, fwd_meta = [tokens], [meta]
        bwd_tok, bwd_meta = [tokens], [meta]
        for hop in range(1, half):
            fwd_meta.append(send(fwd_meta[-1], plus))
            bwd_meta.append(send(bwd_meta[-1], minus))
            fwd_tok.append(send(fwd_tok[-1], plus))
            bwd_tok.append(send(bwd_tok[-1], minus))
        far_meta = send(fwd_meta[-1], plus)
        far_tok = jnp.concatenate([send(fwd_tok[-1][:half_tok], plus), send(bwd_tok[-1][half_tok:], minus)], axis=0)

        def relative(m):
            c = m[:top_k].astype(jnp.int32)
            rel = c - z * chip_rows
            inside = (c >= 0) & (rel >= 0) & (rel < chip_rows)
            rel = (rel - core * core_rows) % chip_rows
            return jnp.where(inside, rel, -1)

        def gather_rows(blocks, metas):
            rel = jnp.stack([relative(m) for m in metas])
            x = jnp.stack(blocks)
            pos = lax.broadcasted_iota(jnp.int32, (len(blocks), chip_rows, tok_count), 1)
            hit = jnp.zeros(pos.shape, jnp.bool_)
            for k in range(top_k):
                hit = hit | (pos == rel[:, k][:, None, :])
            sel = hit.astype(jnp.bfloat16)
            return jnp.einsum('nst,ntd->nsd', sel, x, preferred_element_type=jnp.float32).astype(jnp.bfloat16)

        def exchange(rows):
            n = rows.shape[0]
            other = send(rows[:, core_rows:], swap)
            both = jnp.concatenate([rows[:, :core_rows], other], axis=0)
            return both.reshape(2 * n, local_experts, capacity, hidden)

        def ffn(rows):
            act_a = jnp.einsum('secd,edf->secf', rows, expert_w1, preferred_element_type=jnp.float32)
            act_b = jnp.einsum('secd,edf->secf', rows, expert_w3, preferred_element_type=jnp.float32)
            h = (jax.nn.silu(act_a) * act_b).astype(jnp.bfloat16)
            return jnp.einsum('secf,efd->secd', h, expert_w2, preferred_element_type=jnp.float32).astype(jnp.bfloat16)

        def give_back(res):
            n = res.shape[0] // 2
            res = res.reshape(2 * n, core_rows, hidden)
            other = send(res[n:], swap)
            return jnp.concatenate([res[:n], other], axis=1)

        def combine(res, metas):
            rel = jnp.stack([relative(m).T for m in metas])
            gate = jnp.stack([m[top_k:2 * top_k].T for m in metas])
            pos = lax.broadcasted_iota(jnp.int32, (len(metas), tok_count, chip_rows), 2)
            w = jnp.zeros(pos.shape, jnp.float32)
            for k in range(top_k):
                w = jnp.where(pos == rel[:, :, k][:, :, None], gate[:, :, k][:, :, None], w)
            hi = lax.reduce_precision(w, 8, 7)
            rest = w - hi
            mid = lax.reduce_precision(rest, 8, 7)
            low = rest - mid
            w3 = jnp.concatenate([hi.astype(jnp.bfloat16), mid.astype(jnp.bfloat16), low.astype(jnp.bfloat16)], axis=2)
            res3 = jnp.concatenate([res, res, res], axis=1)
            return jnp.einsum('nts,nsd->ntd', w3, res3, preferred_element_type=jnp.float32)

        gate_logit = jnp.dot(tokens, shared_gate, preferred_element_type=jnp.float32)
        shared_a = jnp.dot(tokens, shared_w1, preferred_element_type=jnp.float32)
        shared_b = jnp.dot(tokens, shared_w3, preferred_element_type=jnp.float32)
        shared_h = (jax.nn.silu(shared_a) * shared_b).astype(jnp.bfloat16)
        shared_out = jnp.dot(shared_h, shared_w2, preferred_element_type=jnp.float32)
        base = tokens.astype(jnp.float32) + jax.nn.sigmoid(gate_logit)[:, None] * shared_out

        part = {}
        order = [0, 1, half] + list(range(half - 1, 1, -1))
        dep = base
        for d in order:
            if d == 0:
                blocks, metas = [tokens], [meta]
            elif d == half:
                blocks, metas = [far_tok], [far_meta]
            else:
                blocks, metas = [bwd_tok[d], fwd_tok[d]], [bwd_meta[d], fwd_meta[d]]
            rows = exchange(gather_rows(blocks, metas))
            rows = after(rows, dep)
            res = ffn(rows)
            dep = res
            part[d] = combine(give_back(res), metas)

        far = part[half][0]
        got_p = send(far[:half_tok], plus)
        got_m = send(far[half_tok:], minus)
        for d in range(half - 1, 0, -1):
            mine_p, mine_m = part[d][0], part[d][1]
            if d == half - 1:
                mine_p = jnp.concatenate([mine_p[:half_tok] + got_p, mine_p[half_tok:]], axis=0)
                mine_m = jnp.concatenate([mine_m[:half_tok], mine_m[half_tok:] + got_m], axis=0)
            else:
                mine_p = mine_p + got_p
                mine_m = mine_m + got_m
            got_p = send(mine_p, plus)
            got_m = send(mine_m, minus)
        total = base + part[0][0] + got_p + got_m
        return total.astype(jnp.bfloat16)

    return jax.shard_map(device_step, mesh=mesh, in_specs=(row_spec, row_spec, row_spec, row_spec, replicated, replicated, replicated, replicated, expert_spec, expert_spec, expert_spec), out_specs=row_spec, check_vma=False)
```

```python
import functools

import jax
import jax.numpy as jnp
from jax import lax
from jax.experimental import pallas as pl
from jax.experimental.pallas import tpu as pltpu
from jax.sharding import PartitionSpec as P

MESH = pl.DeviceIdType.MESH
F32 = jnp.float32
BF16 = jnp.bfloat16


def chunks(total, width):
    return [(start, min(width, total - start)) for start in range(0, total, width)]


def moe_kernel(num_ep, top_k, capacity,
               tok_hbm, meta_hbm, gate_ref, ws1, ws3, ws2, we1, we3, we2,
               out_ref,
               tok, meta, w1a, w1b, w3a, w3b, w2s, xbuf, xsend, rbuf, rrecv, hbuf, part, rs, base,
               load_sem, ab_sem, w2_sem,
               first_send, first_recv, second_send, second_recv, meta_send, meta_recv,
               x_send, x_recv, r_send, r_recv, rs_send, rs_recv, credit):
    tokens, hidden = tok.shape[1:]
    experts = we1.shape[0]
    ff = we1.shape[2]
    ff_a, ff_b = w1a.shape[1], w1b.shape[1]
    half_tok = tokens // 2
    nz = num_ep // 2
    far = nz // 2
    core_rows = experts * capacity
    chip_rows = 2 * core_rows
    pieces = 4
    piece = tokens // pieces
    quarter = half_tok // 2

    ep = lax.axis_index('ep')
    z, core = ep // 2, ep % 2
    right = (ep + 2) % num_ep
    left = (ep + num_ep - 2) % num_ep
    partner = z * 2 + 1 - core
    towards = (right, left)
    origin = (left, right)

    barrier = pltpu.get_barrier_semaphore()
    for other in (left, right, partner):
        pl.semaphore_signal(barrier, inc=1, device_id={'ep': other}, device_id_type=MESH)

    load_tok = pltpu.make_async_copy(tok_hbm, tok.at[0], load_sem.at[0])
    load_meta = pltpu.make_async_copy(meta_hbm, meta.at[0], load_sem.at[1])
    load_tok.start()
    load_meta.start()

    def ab_copies(which, m1, m3, lead, col):
        lo, width = (0, ff_a) if which == 0 else (ff_a, ff_b)
        dst1, dst3 = (w1a, w3a) if which == 0 else (w1b, w3b)
        cols = pl.ds(col + lo, width)
        src1 = m1.at[lead, :, cols] if lead is not None else m1.at[:, cols]
        src3 = m3.at[lead, :, cols] if lead is not None else m3.at[:, cols]
        return (pltpu.make_async_copy(src1, dst1, ab_sem.at[which, 0]),
                pltpu.make_async_copy(src3, dst3, ab_sem.at[which, 1]))

    def start_ab(which, e):
        for c in ab_copies(which, we1, we3, e, 0):
            c.start()

    def start_shared_ab(which, i):
        for c in ab_copies(which, ws1, ws3, None, i * ff):
            c.start()

    def wait_ab(which):
        for c in ab_copies(which, we1, we3, 0, 0):
            c.wait()

    def w2_copy(e, slot):
        return pltpu.make_async_copy(we2.at[e], w2s.at[slot], w2_sem.at[slot])

    def shared_w2_copy(i, slot):
        return pltpu.make_async_copy(ws2.at[pl.ds(i * ff, ff)], w2s.at[slot], w2_sem.at[slot])

    start_ab(0, 0)
    start_ab(1, 0)
    w2_copy(0, 0).start()
    w2_copy(1, 1).start()
    load_tok.wait()
    load_meta.wait()
    pl.semaphore_wait(barrier, 3)

    def slot_of(direction, d):
        if d == 0:
            return 0
        if d == far:
            return 2 * far - 1
        return d if direction == 0 else far - 1 + d

    def remote(src, dst, send_sem, recv_sem, device):
        return pltpu.make_async_remote_copy(src_ref=src, dst_ref=dst, send_sem=send_sem, recv_sem=recv_sem,
                                            device_id={'ep': device}, device_id_type=MESH)

    def first_copy(direction, d, q):
        rows = pl.ds((0 if direction == 0 else half_tok) + q * quarter, quarter)
        return remote(tok.at[slot_of(direction, d - 1), rows], tok.at[slot_of(direction, d), rows],
                      first_send.at[direction, d - 1, q], first_recv.at[direction, d - 1, q], towards[direction])

    def second_copy(direction, d):
        rows = pl.ds(half_tok if direction == 0 else 0, half_tok)
        return remote(tok.at[slot_of(direction, d - 1), rows], tok.at[slot_of(direction, d), rows],
                      second_send.at[direction, d - 1], second_recv.at[direction, d - 1], towards[direction])

    def meta_copy(direction, d):
        return remote(meta.at[slot_of(direction, d - 1)], meta.at[slot_of(direction, d)],
                      meta_send.at[direction, d - 1], meta_recv.at[direction, d - 1], towards[direction])

    def meta_hops(direction):
        return far if direction == 0 else far - 1

    for direction in (0, 1):
        meta_copy(direction, 1).start()
        for q in (0, 1):
            first_copy(direction, 1, q).start()
    for d in range(1, far):
        for direction in (0, 1):
            meta_copy(direction, d).wait_recv()
            if d + 1 <= meta_hops(direction):
                meta_copy(direction, d + 1).start()
        for q in (0, 1):
            for direction in (0, 1):
                first_copy(direction, d, q).wait_recv()
                first_copy(direction, d + 1, q).start()
    for direction in (0, 1):
        second_copy(direction, 1).start()
    meta_copy(0, far).wait_recv()
    for q in (0, 1):
        for direction in (0, 1):
            first_copy(direction, far, q).wait_recv()

    def second_step(d):
        for direction in (0, 1):
            second_copy(direction, d).wait_recv()
            if d + 1 < far:
                second_copy(direction, d + 1).start()

    my_base = (z * chip_rows).astype(F32)
    my_core = (core * core_rows).astype(F32)

    def relative(slot):
        code = meta[slot, 0:top_k, :]
        rel = code - my_base
        inside = (code >= 0.0) & (rel >= 0.0) & (rel < float(chip_rows))
        rel = rel - my_core
        rel = jnp.where(rel < 0.0, rel + float(chip_rows), rel)
        return jnp.where(inside, rel, -1.0)

    def position():
        return lax.broadcasted_iota(jnp.int32, (chip_rows, tokens), 0).astype(F32)

    def gather(i, slot):
        rel = relative(slot)
        pos = position()
        sel = jnp.zeros((chip_rows, tokens), F32)
        for k in range(top_k):
            sel = jnp.where(pos == rel[k:k + 1, :], 1.0, sel)
        sel = sel.astype(BF16)
        for n0, nw in chunks(hidden, 512):
            rows = jnp.dot(sel, tok[slot, :, n0:n0 + nw], preferred_element_type=F32).astype(BF16)
            xbuf[i, :, n0:n0 + nw] = rows[:core_rows]
            xsend[i, :, n0:n0 + nw] = rows[core_rows:]

    def combine(i, slot, dst):
        rel = relative(slot)
        gates = meta[slot, top_k:2 * top_k, :]
        pos = position()
        w = jnp.zeros((chip_rows, tokens), F32)
        for k in range(top_k):
            w = jnp.where(pos == rel[k:k + 1, :], gates[k:k + 1, :], w)
        w = w.T
        hi = w.astype(BF16)
        rest = w - hi.astype(F32)
        mid = rest.astype(BF16)
        low = (rest - mid.astype(F32)).astype(BF16)
        for n0, nw in chunks(hidden, 256):
            res = jnp.concatenate([rbuf[i, :, n0:n0 + nw], rrecv[i, :, n0:n0 + nw]], axis=0)
            acc = jnp.dot(hi, res, preferred_element_type=F32)
            acc = acc + jnp.dot(mid, res, preferred_element_type=F32)
            acc = acc + jnp.dot(low, res, preferred_element_type=F32)
            dst[:, n0:n0 + nw] = acc

    def up_half(x_of, rows, which):
        lo, width = (0, ff_a) if which == 0 else (ff_a, ff_b)
        m1, m3 = (w1a, w3a) if which == 0 else (w1b, w3b)
        x = x_of()
        for n0, nw in chunks(width, 256):
            a = jnp.dot(x, m1[:, n0:n0 + nw], preferred_element_type=F32)
            b = jnp.dot(x, m3[:, n0:n0 + nw], preferred_element_type=F32)
            hbuf[0:rows, lo + n0:lo + n0 + nw] = (jax.nn.silu(a) * b).astype(BF16)

    def expert_loop(phase_srcs, last, extra):
        rows = capacity * len(phase_srcs)

        def body(e, carry):
            row0 = pl.multiple_of(e * capacity, 16)
            nxt = (e + 1) % experts

            def x_of():
                return jnp.concatenate([xbuf[s, pl.ds(row0, capacity), :] for s in phase_srcs], axis=0)

            for which in (0, 1):
                wait_ab(which)
                up_half(x_of, rows, which)
                if last:
                    @pl.when(e < experts - 1)
                    def _():
                        start_ab(which, nxt)

                    @pl.when(e == experts - 1)
                    def _():
                        start_shared_ab(which, 0)
                else:
                    start_ab(which, nxt)
            slot = e % 2
            w2_copy(0, slot).wait()
            for n0, nw in chunks(hidden, 256):
                r = jnp.dot(hbuf[0:rows, :], w2s[slot, :, n0:n0 + nw], preferred_element_type=F32).astype(BF16)
                for j, s in enumerate(phase_srcs):
                    rbuf[s, pl.ds(row0, capacity), n0:n0 + nw] = r[j * capacity:(j + 1) * capacity]
            if last:
                @pl.when(e < experts - 2)
                def _():
                    w2_copy(e + 2, slot).start()

                for i in (0, 1):
                    @pl.when(e == experts - 2 + i)
                    def _():
                        shared_w2_copy(i, i).start()
            else:
                w2_copy((e + 2) % experts, slot).start()
            if extra is not None:
                extra(e)
            return carry

        lax.fori_loop(0, experts, body, 0)

    def x_copy(phase, n):
        return remote(xsend.at[pl.ds(0, n)], xbuf.at[pl.ds(2, n)], x_send.at[phase], x_recv.at[phase], partner)

    def r_copy(phase, n):
        return remote(rbuf.at[pl.ds(2, n)], rrecv.at[pl.ds(0, n)], r_send.at[phase], r_recv.at[phase], partner)

    def run_phase(phase, slots, dsts, last=False, extra=None, before_combine=None):
        n = len(slots)
        for i, slot in enumerate(slots):
            gather(i, slot)
        x_copy(phase, n).start()
        x_copy(phase, n).wait()
        expert_loop([0, 2] if n == 1 else [0, 1, 2, 3], last, extra)
        r_copy(phase, n).start()
        r_copy(phase, n).wait()
        if before_combine is not None:
            before_combine()
        for i, slot in enumerate(slots):
            combine(i, slot, dsts[i])

    def rs_copy(direction, hop, rows_piece):
        rows = pl.ds(pl.multiple_of(rows_piece * piece, 8), piece)
        if hop == 1:
            src = part.at[0, 0, rows]
        else:
            src = part.at[(hop - 1) % 2, direction, rows]
        return remote(src, rs.at[direction, (hop - 1) % 2, rows],
                      rs_send.at[direction, hop - 1, rows_piece], rs_recv.at[direction, hop - 1, rows_piece],
                      towards[direction])

    def first_pieces(direction):
        return (0, 1) if direction == 0 else (2, 3)

    def forward(direction, hop, p, add):
        rows = pl.ds(pl.multiple_of(p * piece, 8), piece)
        if add:
            rs_copy(direction, hop - 1, p).wait_recv()
            mine = part.at[(hop - 1) % 2, direction, rows]
            mine[...] = mine[...] + rs[direction, hop % 2, rows, :]
        rs_copy(direction, hop, p).start()

    def give_credit(which):
        for direction in (0, 1):
            pl.semaphore_signal(credit.at[direction, which], inc=1, device_id={'ep': origin[direction]}, device_id_type=MESH)

    def take_credit(which):
        for direction in (0, 1):
            pl.semaphore_wait(credit.at[direction, which], 1)

    def wait_sends(hop):
        for direction in (0, 1):
            for p in (first_pieces(direction) if hop == 1 else range(pieces)):
                rs_copy(direction, hop, p).wait_send()

    def gather_service(e):
        for step in range(1, far - 1):
            @pl.when(e == 2 * (step - 1))
            def _():
                second_step(step)

    run_phase(0, [slot_of(0, far)], [part.at[0, 0]], extra=gather_service)
    for direction in (0, 1):
        for p in first_pieces(direction):
            rs_copy(direction, 1, p).start()
    second_step(far - 1)

    def pair(d):
        return [slot_of(1, d), slot_of(0, d)]

    run_phase(1, pair(far - 1), [part.at[1, 0], part.at[1, 1]])
    for j in (0, 1):
        for direction in (0, 1):
            forward(direction, 2, first_pieces(direction)[j], True)
    give_credit(0)
    for j in (0, 1):
        for direction in (0, 1):
            forward(direction, 2, first_pieces(1 - direction)[j], False)

    run_phase(2, pair(far - 2), [part.at[0, 0], part.at[0, 1]], before_combine=lambda: wait_sends(1))
    take_credit(0)

    def service(hop):
        def run(e):
            for direction in (0, 1):
                forward(direction, hop, e, True)
        return run

    run_phase(3, pair(far - 3), [part.at[1, 0], part.at[1, 1]], extra=service(3), before_combine=lambda: wait_sends(2))
    give_credit(1)
    take_credit(1)

    run_phase(4, [0], [base], last=True, extra=service(4))

    x_all = tok[0].astype(F32) * gate_ref[...].astype(F32)
    scale = jax.nn.sigmoid(jnp.sum(x_all, axis=1, keepdims=True))

    def shared_body(i, carry):
        for which in (0, 1):
            wait_ab(which)
            up_half(lambda: tok[0], tokens, which)

            @pl.when(i == 0)
            def _():
                start_shared_ab(which, 1)
        w2_copy(0, i).wait()
        for n0, nw in chunks(hidden, 256):
            s = jnp.dot(hbuf[0:tokens, :], w2s[i, :, n0:n0 + nw], preferred_element_type=F32)
            base[:, n0:n0 + nw] = base[:, n0:n0 + nw] + scale * s
        return carry

    lax.fori_loop(0, 2, shared_body, 0)

    def finish(p, carry):
        rows = pl.ds(pl.multiple_of(p * piece, 16), piece)
        total = tok[0, rows, :].astype(F32) + base[rows, :]
        for direction in (0, 1):
            rs_copy(direction, far, p).wait_recv()
            total = total + rs[direction, (far - 1) % 2, rows, :]
        out_ref[rows, :] = total.astype(BF16)
        return carry

    lax.fori_loop(0, pieces, finish, 0)

    for direction in (0, 1):
        for d in range(1, far + 1):
            for q in (0, 1):
                first_copy(direction, d, q).wait_send()
            if d < far:
                second_copy(direction, d).wait_send()
            if d <= meta_hops(direction):
                meta_copy(direction, d).wait_send()
    wait_sends(3)
    wait_sends(4)


def solution(mesh):
    num_ep = mesh.shape['ep']
    row_spec = P(('dp', 'ep'), None)
    replicated = P()
    expert_spec = P('ep', None, None)

    def device_step(tokens, expert_ids, gate_vals, slots, shared_w1, shared_w3, shared_w2, shared_gate, expert_w1, expert_w3, expert_w2):
        tok_count, hidden = tokens.shape
        top_k = expert_ids.shape[1]
        experts, _, ff = expert_w1.shape
        num_experts = experts * num_ep
        capacity = 8 * ((2 * tok_count * top_k + 8 * num_experts - 1) // (8 * num_experts))
        core_rows = experts * capacity
        far = num_ep // 4
        ff_a = 256 * ((ff + 511) // 512)
        ff_b = ff - ff_a

        code = jnp.where(slots >= 0, expert_ids * capacity + slots, -1).astype(F32)
        meta = jnp.concatenate([code, gate_vals, jnp.zeros((tok_count, 16 - 2 * top_k), F32)], axis=1).T

        vmem = pl.BlockSpec(memory_space=pltpu.VMEM)
        hbm = pl.BlockSpec(memory_space=pl.ANY)
        dma = pltpu.SemaphoreType.DMA
        return pl.pallas_call(
            functools.partial(moe_kernel, num_ep, top_k, capacity),
            out_shape=jax.ShapeDtypeStruct((tok_count, hidden), BF16),
            in_specs=[hbm, hbm, vmem] + [hbm] * 6,
            out_specs=vmem,
            scratch_shapes=[
                pltpu.VMEM((2 * far, tok_count, hidden), BF16),
                pltpu.VMEM((2 * far, 16, tok_count), F32),
                pltpu.VMEM((hidden, ff_a), BF16),
                pltpu.VMEM((hidden, ff_b), BF16),
                pltpu.VMEM((hidden, ff_a), BF16),
                pltpu.VMEM((hidden, ff_b), BF16),
                pltpu.VMEM((2, ff, hidden), BF16),
                pltpu.VMEM((4, core_rows, hidden), BF16),
                pltpu.VMEM((2, core_rows, hidden), BF16),
                pltpu.VMEM((4, core_rows, hidden), BF16),
                pltpu.VMEM((2, core_rows, hidden), BF16),
                pltpu.VMEM((tok_count, ff), BF16),
                pltpu.VMEM((2, 2, tok_count, hidden), F32),
                pltpu.VMEM((2, 2, tok_count, hidden), F32),
                pltpu.VMEM((tok_count, hidden), F32),
                dma((2,)), dma((2, 2)), dma((2,)),
                dma((2, far, 2)), dma((2, far, 2)), dma((2, far)), dma((2, far)), dma((2, far)), dma((2, far)),
                dma((far + 1,)), dma((far + 1,)), dma((far + 1,)), dma((far + 1,)),
                dma((2, far, 4)), dma((2, far, 4)), pltpu.SemaphoreType.REGULAR((2, 2)),
            ],
            compiler_params=pltpu.CompilerParams(collective_id=0, has_side_effects=True, vmem_limit_bytes=66_000_000),
        )(tokens, meta, shared_gate.reshape(1, hidden), shared_w1, shared_w3, shared_w2, expert_w1, expert_w3, expert_w2)

    return jax.shard_map(device_step, mesh=mesh, in_specs=(row_spec, row_spec, row_spec, row_spec, replicated, replicated, replicated, replicated, expert_spec, expert_spec, expert_spec), out_specs=row_spec, check_vma=False)
```

```python
import functools

import jax
import jax.numpy as jnp
from jax import lax
from jax.experimental import pallas as pl
from jax.experimental.pallas import tpu as pltpu
from jax.sharding import PartitionSpec as P

MESH = pl.DeviceIdType.MESH
F32 = jnp.float32
BF16 = jnp.bfloat16


def chunks(total, width):
    return [(start, min(width, total - start)) for start in range(0, total, width)]


def moe_kernel(num_ep, capacity,
               tok_hbm, ids_ref, slots_ref, gates_ref, gate_ref, ws1, ws3, ws2, we1, we3, we2,
               out_ref,
               tok, meta, w1a, w1b, w3a, w3b, w2s, xbuf, xsend, rbuf, rrecv, hbuf, part, rs, base,
               load_sem, ab_sem, w2_sem,
               first_send, first_recv, second_send, second_recv, meta_send, meta_recv,
               x_send, x_recv, r_send, r_recv, rs_send, rs_recv, credit):
    scope = jax.named_scope
    tokens, hidden = tok.shape[1:]
    top_k = ids_ref.shape[0]
    experts = we1.shape[0]
    ff = we1.shape[2]
    ff_a, ff_b = w1a.shape[1], w1b.shape[1]
    half_tok = tokens // 2
    nz = num_ep // 2
    far = nz // 2
    core_rows = experts * capacity
    chip_rows = 2 * core_rows
    pieces = rs_send.shape[2]
    width = hidden // pieces
    firsts = first_send.shape[2]
    first_rows = half_tok // firsts
    seconds = second_send.shape[2]
    second_rows = half_tok // seconds

    ep = lax.axis_index('ep')
    z, core = ep // 2, ep % 2
    right = (ep + 2) % num_ep
    left = (ep + num_ep - 2) % num_ep
    partner = z * 2 + 1 - core
    towards = (right, left)
    origin = (left, right)
    both = (0, 1)

    barrier = pltpu.get_barrier_semaphore()
    for other in (left, right, partner):
        pl.semaphore_signal(barrier, inc=1, device_id={'ep': other}, device_id_type=MESH)

    load_tok = pltpu.make_async_copy(tok_hbm, tok.at[0], load_sem.at[0])
    load_tok.start()
    meta[0, 0:top_k, :] = jnp.where(slots_ref[...] >= 0, ids_ref[...] * capacity + slots_ref[...], -1).astype(F32)
    meta[0, 8:8 + top_k, :] = gates_ref[...]

    def ab_copies(which, m1, m3, lead, col):
        lo, span = (0, ff_a) if which == 0 else (ff_a, ff_b)
        dst1, dst3 = (w1a, w3a) if which == 0 else (w1b, w3b)
        cols = pl.ds(col + lo, span)
        src1 = m1.at[lead, :, cols] if lead is not None else m1.at[:, cols]
        src3 = m3.at[lead, :, cols] if lead is not None else m3.at[:, cols]
        return (pltpu.make_async_copy(src1, dst1, ab_sem.at[which, 0]),
                pltpu.make_async_copy(src3, dst3, ab_sem.at[which, 1]))

    def start_ab(which, e):
        for c in ab_copies(which, we1, we3, e, 0):
            c.start()

    def start_shared_ab(which, i):
        for c in ab_copies(which, ws1, ws3, None, i * ff):
            c.start()

    def wait_ab(which):
        for c in ab_copies(which, we1, we3, 0, 0):
            c.wait()

    def w2_copy(e, slot):
        return pltpu.make_async_copy(we2.at[e], w2s.at[slot], w2_sem.at[slot])

    def shared_w2_copy(i, slot):
        return pltpu.make_async_copy(ws2.at[pl.ds(i * ff, ff)], w2s.at[slot], w2_sem.at[slot])

    def slot_of(direction, d):
        if d == 0:
            return 0
        if d == far:
            return 2 * far - 1
        return d if direction == 0 else far - 1 + d

    def remote(src, dst, send_sem, recv_sem, device):
        return pltpu.make_async_remote_copy(src_ref=src, dst_ref=dst, send_sem=send_sem, recv_sem=recv_sem,
                                            device_id={'ep': device}, device_id_type=MESH)

    def first_copy(direction, d, q):
        rows = pl.ds((0 if direction == 0 else half_tok) + q * first_rows, first_rows)
        return remote(tok.at[slot_of(direction, d - 1), rows], tok.at[slot_of(direction, d), rows],
                      first_send.at[direction, d - 1, q], first_recv.at[direction, d - 1, q], towards[direction])

    def second_copy(direction, d, q):
        rows = pl.ds((half_tok if direction == 0 else 0) + q * second_rows, second_rows)
        return remote(tok.at[slot_of(direction, d - 1), rows], tok.at[slot_of(direction, d), rows],
                      second_send.at[direction, d - 1, q], second_recv.at[direction, d - 1, q], towards[direction])

    def meta_copy(direction, d):
        return remote(meta.at[slot_of(direction, d - 1)], meta.at[slot_of(direction, d)],
                      meta_send.at[direction, d - 1], meta_recv.at[direction, d - 1], towards[direction])

    def meta_hops(direction):
        return far if direction == 0 else far - 1

    with scope('load'):
        load_tok.wait()
    with scope('barrier'):
        pl.semaphore_wait(barrier, 3)
    for q in range(firsts):
        for direction in both:
            first_copy(direction, 1, q).start()
            if q == 0:
                meta_copy(direction, 1).start()
    start_ab(0, 0)
    start_ab(1, 0)
    w2_copy(0, 0).start()
    w2_copy(1, 1).start()
    for d in range(1, far):
        with scope('ag_hop'):
            for q in range(firsts):
                for direction in both:
                    first_copy(direction, d, q).wait_recv()
                    first_copy(direction, d + 1, q).start()
                    if q == 0:
                        meta_copy(direction, d).wait_recv()
                        if d + 1 <= meta_hops(direction):
                            meta_copy(direction, d + 1).start()
    for q in range(seconds):
        for direction in both:
            second_copy(direction, 1, q).start()
    with scope('ag_far'):
        meta_copy(0, far).wait_recv()
        for q in range(firsts):
            for direction in both:
                first_copy(direction, far, q).wait_recv()

    def second_step(d, q):
        with scope('second_step'):
            for direction in both:
                second_copy(direction, d, q).wait_recv()
                if d + 1 < far:
                    second_copy(direction, d + 1, q).start()

    my_base = (z * chip_rows).astype(F32)
    my_core = (core * core_rows).astype(F32)

    def relative(slot):
        code = meta[slot, 0:top_k, :]
        rel = code - my_base
        inside = (code >= 0.0) & (rel >= 0.0) & (rel < float(chip_rows))
        rel = rel - my_core
        rel = jnp.where(rel < 0.0, rel + float(chip_rows), rel)
        return jnp.where(inside, rel, -1.0)

    def position():
        return lax.broadcasted_iota(jnp.int32, (chip_rows, tokens), 0).astype(F32)

    def gather(i, slot):
        rel = relative(slot)
        pos = position()
        sel = jnp.zeros((chip_rows, tokens), F32)
        for k in range(top_k):
            sel = jnp.where(pos == rel[k:k + 1, :], 1.0, sel)
        sel = sel.astype(BF16)
        for n0, nw in chunks(hidden, 512):
            rows = jnp.dot(sel, tok[slot, :, n0:n0 + nw], preferred_element_type=F32).astype(BF16)
            xbuf[i, :, n0:n0 + nw] = rows[:core_rows]
            xsend[i, :, n0:n0 + nw] = rows[core_rows:]

    def weights_of(slot):
        rel = relative(slot)
        gates = meta[slot, 8:8 + top_k, :]
        pos = position()
        w = jnp.zeros((chip_rows, tokens), F32)
        for k in range(top_k):
            w = jnp.where(pos == rel[k:k + 1, :], gates[k:k + 1, :], w)
        w = w.T
        hi = w.astype(BF16)
        rest = w - hi.astype(F32)
        mid = rest.astype(BF16)
        low = (rest - mid.astype(F32)).astype(BF16)
        return hi, mid, low

    def combine(i, terms, dst, p):
        for n0, nw in chunks(width, 256):
            n0 = p * width + n0
            res = jnp.concatenate([rbuf[i, :, n0:n0 + nw], rrecv[i, :, n0:n0 + nw]], axis=0)
            acc = jnp.dot(terms[0], res, preferred_element_type=F32)
            for term in terms[1:]:
                acc = acc + jnp.dot(term, res, preferred_element_type=F32)
            dst[:, n0:n0 + nw] = acc

    def up_part(x_of, rows, which):
        lo, span = (0, ff_a) if which == 0 else (ff_a, ff_b)
        m1, m3 = (w1a, w3a) if which == 0 else (w1b, w3b)
        x = x_of()
        for n0, nw in chunks(span, 256):
            a = jnp.dot(x, m1[:, n0:n0 + nw], preferred_element_type=F32)
            b = jnp.dot(x, m3[:, n0:n0 + nw], preferred_element_type=F32)
            hbuf[0:rows, lo + n0:lo + n0 + nw] = (jax.nn.silu(a) * b).astype(BF16)

    def x_copy(phase, i):
        return remote(xsend.at[i], xbuf.at[2 + i], x_send.at[phase, i], x_recv.at[phase, i], partner)

    def r_copy(phase, e):
        rows = pl.ds(pl.multiple_of(e * capacity, 16), capacity)
        return remote(rbuf.at[pl.ds(2, 2), rows], rrecv.at[:, rows], r_send.at[phase, e], r_recv.at[phase, e], partner)

    def expert_loop(phase, last, extra):
        def body(e, carry):
            row0 = pl.multiple_of(e * capacity, 16)
            nxt = (e + 1) % experts

            def x_of():
                return jnp.concatenate([xbuf[s, pl.ds(row0, capacity), :] for s in range(4)], axis=0)

            for which in both:
                with scope('wait_ab'):
                    wait_ab(which)
                with scope('up'):
                    up_part(x_of, 4 * capacity, which)
                if last:
                    @pl.when(e < experts - 1)
                    def _():
                        start_ab(which, nxt)

                    @pl.when(e == experts - 1)
                    def _():
                        start_shared_ab(which, 0)
                else:
                    start_ab(which, nxt)
                if extra is not None:
                    extra(e, which)
            slot = e % 2
            with scope('wait_w2'):
                w2_copy(0, slot).wait()
            with scope('down'):
                for n0, nw in chunks(hidden, 256):
                    r = jnp.dot(hbuf[0:4 * capacity, :], w2s[slot, :, n0:n0 + nw], preferred_element_type=F32).astype(BF16)
                    for s in range(4):
                        rbuf[s, pl.ds(row0, capacity), n0:n0 + nw] = r[s * capacity:(s + 1) * capacity]
            r_copy(phase, e).start()
            if last:
                @pl.when(e < experts - 2)
                def _():
                    w2_copy(e + 2, slot).start()

                for i in both:
                    @pl.when(e == experts - 2 + i)
                    def _():
                        shared_w2_copy(i, i).start()
            else:
                w2_copy((e + 2) % experts, slot).start()
            if extra is not None:
                extra(e, 2)
            return carry

        with scope('experts'):
            lax.fori_loop(0, experts, body, 0)

    def run_experts(phase, slots, last=False, extra=None):
        with scope('gather'):
            for i in both:
                gather(i, slots[i])
                x_copy(phase, i).start()
        with scope('x_swap'):
            for i in both:
                x_copy(phase, i).wait()
        expert_loop(phase, last, extra)
        with scope('weights'):
            terms = [weights_of(slot) for slot in slots]
        with scope('r_swap'):
            for e in range(experts):
                r_copy(phase, e).wait()
        return terms

    def rs_copy(direction, hop, p):
        cols = pl.ds(p * width if isinstance(p, int) else pl.multiple_of(p * width, 128), width)
        src = part.at[0, 0, :, cols] if hop == 1 else part.at[(hop - 1) % 2, direction, :, cols]
        return remote(src, rs.at[direction, (hop - 1) % 2, :, cols],
                      rs_send.at[direction, hop - 1, p], rs_recv.at[direction, hop - 1, p], towards[direction])

    def first_pieces(direction):
        half = pieces // 2
        return range(0, half) if direction == 0 else range(half, pieces)

    def order(direction, j):
        return (j + pieces // 2) % pieces if direction == 0 else j

    def forward(direction, hop, p, add):
        if add:
            rs_copy(direction, hop - 1, p).wait_recv()
            cols = pl.ds(p * width if isinstance(p, int) else pl.multiple_of(p * width, 128), width)
            mine = part.at[(hop - 1) % 2, direction, :, cols]
            mine[...] = mine[...] + rs[direction, hop % 2, :, cols]
        rs_copy(direction, hop, p).start()

    def give_credit(which):
        for direction in both:
            pl.semaphore_signal(credit.at[direction, which], inc=1, device_id={'ep': origin[direction]}, device_id_type=MESH)

    def take_credit(which):
        for direction in both:
            pl.semaphore_wait(credit.at[direction, which], 1)

    def wait_sends(hop):
        with scope('wait_sends'):
            for direction in both:
                for p in (first_pieces(direction) if hop == 1 else range(pieces)):
                    rs_copy(direction, hop, p).wait_send()

    def pair(d):
        return [slot_of(1, d), slot_of(0, d)]

    points = ((0, 2), (2, 0), (3, 1))

    def gather_service(e, stage):
        for n, (at_e, at_stage) in enumerate(points):
            if stage == at_stage:
                @pl.when(e == at_e)
                def _():
                    second_step(1 + n // seconds, n % seconds)

    terms = run_experts(0, [slot_of(0, far), 0], extra=gather_service)
    steps = [(d, q) for d in range(1, far) for q in range(seconds)]
    before = (far - 2) * seconds
    with scope('combine'):
        for p in range(pieces):
            combine(0, terms[0], part.at[0, 0], p)
    for d, q in steps[len(points):before]:
        second_step(d, q)
    for j in range(pieces // 2):
        for direction in both:
            rs_copy(direction, 1, first_pieces(direction)[j]).start()
    with scope('combine'):
        for p in range(pieces):
            combine(1, terms[1], base, p)
    for d, q in steps[before:]:
        second_step(d, q)

    terms = run_experts(1, pair(far - 1))
    with scope('combine'):
        for j in range(pieces):
            for direction in both:
                p = order(direction, j)
                combine(direction, terms[direction], part.at[1, direction], p)
                forward(direction, 2, p, p in first_pieces(direction))
    give_credit(0)

    terms = run_experts(2, pair(far - 2))
    wait_sends(1)
    with scope('combine'):
        for p in range(pieces):
            for direction in both:
                combine(direction, terms[direction], part.at[0, direction], p)
    take_credit(0)

    def service(e, stage):
        if stage == 2:
            with scope('extra'):
                for direction in both:
                    forward(direction, 3, order(direction, e), True)

    terms = run_experts(3, pair(far - 3), last=True, extra=service)
    give_credit(1)
    wait_sends(2)
    with scope('combine'):
        for p in range(pieces):
            for direction in both:
                combine(direction, terms[direction], part.at[1, direction], p)

    x_all = tok[0].astype(F32) * gate_ref[...].astype(F32)
    scale = jax.nn.sigmoid(jnp.sum(x_all, axis=1, keepdims=True))

    def shared_body(i, carry):
        for which in both:
            wait_ab(which)
            up_part(lambda: tok[0], tokens, which)

            @pl.when(i == 0)
            def _():
                start_shared_ab(which, 1)
        w2_copy(0, i).wait()
        for n0, nw in chunks(hidden, 256):
            s = jnp.dot(hbuf[0:tokens, :], w2s[i, :, n0:n0 + nw], preferred_element_type=F32)
            base[:, n0:n0 + nw] = base[:, n0:n0 + nw] + scale * s
        return carry

    with scope('shared'):
        lax.fori_loop(0, 2, shared_body, 0)

    take_credit(1)
    with scope('last_hop'):
        for j in range(pieces):
            for direction in both:
                forward(direction, far, order(direction, j), True)

    with scope('finish'):
        half = pieces // 2
        for j in range(half):
            for p in (j, j + half):
                cols = pl.ds(p * width, width)
                total = tok[0, :, cols].astype(F32) + base[:, cols]
                for direction in both:
                    rs_copy(direction, far, p).wait_recv()
                    total = total + rs[direction, (far - 1) % 2, :, cols]
                out_ref[:, cols] = total.astype(BF16)

    for direction in both:
        for d in range(1, far + 1):
            for q in range(firsts):
                first_copy(direction, d, q).wait_send()
            if d < far:
                for q in range(seconds):
                    second_copy(direction, d, q).wait_send()
            if d <= meta_hops(direction):
                meta_copy(direction, d).wait_send()
    wait_sends(3)
    wait_sends(4)


def solution(mesh):
    num_ep = mesh.shape['ep']
    row_spec = P(('dp', 'ep'), None)
    replicated = P()
    expert_spec = P('ep', None, None)

    def device_step(tokens, expert_ids, gate_vals, slots, shared_w1, shared_w3, shared_w2, shared_gate, expert_w1, expert_w3, expert_w2):
        tok_count, hidden = tokens.shape
        top_k = expert_ids.shape[1]
        experts, _, ff = expert_w1.shape
        num_experts = experts * num_ep
        capacity = 8 * ((2 * tok_count * top_k + 8 * num_experts - 1) // (8 * num_experts))
        core_rows = experts * capacity
        far = num_ep // 4
        ff_a = 256 * ((ff + 511) // 512)
        ff_b = ff - ff_a

        vmem = pl.BlockSpec(memory_space=pltpu.VMEM)
        hbm = pl.BlockSpec(memory_space=pl.ANY)
        dma = pltpu.SemaphoreType.DMA
        return pl.pallas_call(
            functools.partial(moe_kernel, num_ep, capacity),
            out_shape=jax.ShapeDtypeStruct((tok_count, hidden), BF16),
            in_specs=[hbm, vmem, vmem, vmem, vmem] + [hbm] * 6,
            out_specs=vmem,
            scratch_shapes=[
                pltpu.VMEM((2 * far, tok_count, hidden), BF16),
                pltpu.VMEM((2 * far, 16, tok_count), F32),
                pltpu.VMEM((hidden, ff_a), BF16),
                pltpu.VMEM((hidden, ff_b), BF16),
                pltpu.VMEM((hidden, ff_a), BF16),
                pltpu.VMEM((hidden, ff_b), BF16),
                pltpu.VMEM((2, ff, hidden), BF16),
                pltpu.VMEM((4, core_rows, hidden), BF16),
                pltpu.VMEM((2, core_rows, hidden), BF16),
                pltpu.VMEM((4, core_rows, hidden), BF16),
                pltpu.VMEM((2, core_rows, hidden), BF16),
                pltpu.VMEM((tok_count, ff), BF16),
                pltpu.VMEM((2, 2, tok_count, hidden), F32),
                pltpu.VMEM((2, 2, tok_count, hidden), F32),
                pltpu.VMEM((tok_count, hidden), F32),
                dma((1,)), dma((2, 2)), dma((2,)),
                dma((2, far, 4)), dma((2, far, 4)), dma((2, far - 1, 2)), dma((2, far - 1, 2)), dma((2, far)), dma((2, far)),
                dma((far, 2)), dma((far, 2)), dma((far, experts)), dma((far, experts)),
                dma((2, far, 4)), dma((2, far, 4)), pltpu.SemaphoreType.REGULAR((2, 2)),
            ],
            compiler_params=pltpu.CompilerParams(collective_id=0, has_side_effects=True, vmem_limit_bytes=66_000_000),
        )(tokens, expert_ids.T, slots.T, gate_vals.T, shared_gate.reshape(1, hidden), shared_w1, shared_w3, shared_w2, expert_w1, expert_w3, expert_w2)

    return jax.shard_map(device_step, mesh=mesh, in_specs=(row_spec, row_spec, row_spec, row_spec, replicated, replicated, replicated, replicated, expert_spec, expert_spec, expert_spec), out_specs=row_spec, check_vma=False)
```

```python
import functools

import jax
import jax.numpy as jnp
from jax import lax
from jax.experimental import pallas as pl
from jax.experimental.pallas import tpu as pltpu
from jax.sharding import PartitionSpec as P

MESH = pl.DeviceIdType.MESH
F32 = jnp.float32
BF16 = jnp.bfloat16


def chunks(total, width):
    return [(start, min(width, total - start)) for start in range(0, total, width)]


def moe_kernel(num_ep, capacity,
               tok_hbm, ids_ref, slots_ref, gates_ref, gate_ref, ws1, ws3, ws2, we1, we3, we2,
               out_ref,
               tok, meta, w1a, w1b, w3a, w3b, w2s, xbuf, xsend, rbuf, rrecv, hbuf, part, rs, base, sels, terms, y,
               load_sem, out_sem, ab_sem, w2_sem,
               first_send, first_recv, second_send, second_recv, meta_send, meta_recv,
               x_send, x_recv, r_send, r_recv, rs_send, rs_recv, credit):
    scope = jax.named_scope
    tokens, hidden = tok.shape[1:]
    top_k = ids_ref.shape[0]
    experts = we1.shape[0]
    ff = we1.shape[2]
    ff_a, ff_b = w1a.shape[1], w1b.shape[1]
    half_tok = tokens // 2
    nz = num_ep // 2
    far = nz // 2
    core_rows = experts * capacity
    chip_rows = 2 * core_rows
    pieces = rs_send.shape[2]
    width = hidden // pieces
    firsts = first_send.shape[2]
    first_rows = half_tok // firsts
    seconds = second_send.shape[2]
    second_rows = half_tok // seconds

    ep = lax.axis_index('ep')
    z, core = ep // 2, ep % 2
    right = (ep + 2) % num_ep
    left = (ep + num_ep - 2) % num_ep
    partner = z * 2 + 1 - core
    towards = (right, left)
    origin = (left, right)
    both = (0, 1)

    barrier = pltpu.get_barrier_semaphore()
    for other in (left, right, partner):
        pl.semaphore_signal(barrier, inc=1, device_id={'ep': other}, device_id_type=MESH)

    load_tok = pltpu.make_async_copy(tok_hbm, tok.at[0], load_sem.at[0])
    load_tok.start()
    meta[0, 0:top_k, :] = jnp.where(slots_ref[...] >= 0, ids_ref[...] * capacity + slots_ref[...], -1).astype(F32)
    meta[0, 8:8 + top_k, :] = gates_ref[...]

    def ab_copies(which, m1, m3, lead, col):
        lo, span = (0, ff_a) if which == 0 else (ff_a, ff_b)
        dst1, dst3 = (w1a, w3a) if which == 0 else (w1b, w3b)
        cols = pl.ds(col + lo, span)
        src1 = m1.at[lead, :, cols] if lead is not None else m1.at[:, cols]
        src3 = m3.at[lead, :, cols] if lead is not None else m3.at[:, cols]
        return (pltpu.make_async_copy(src1, dst1, ab_sem.at[which, 0]),
                pltpu.make_async_copy(src3, dst3, ab_sem.at[which, 1]))

    def start_ab(which, e):
        for c in ab_copies(which, we1, we3, e, 0):
            c.start()

    def start_shared_ab(which, i):
        for c in ab_copies(which, ws1, ws3, None, i * ff):
            c.start()

    def wait_ab(which):
        for c in ab_copies(which, we1, we3, 0, 0):
            c.wait()

    def w2_copy(e, slot):
        return pltpu.make_async_copy(we2.at[e], w2s.at[slot], w2_sem.at[slot])

    def shared_w2_copy(i, slot):
        return pltpu.make_async_copy(ws2.at[pl.ds(i * ff, ff)], w2s.at[slot], w2_sem.at[slot])

    def slot_of(direction, d):
        if d == 0:
            return 0
        if d == far:
            return 2 * far - 1
        return d if direction == 0 else far - 1 + d

    def remote(src, dst, send_sem, recv_sem, device):
        return pltpu.make_async_remote_copy(src_ref=src, dst_ref=dst, send_sem=send_sem, recv_sem=recv_sem,
                                            device_id={'ep': device}, device_id_type=MESH)

    def first_copy(direction, d, q):
        rows = pl.ds((0 if direction == 0 else half_tok) + q * first_rows, first_rows)
        return remote(tok.at[slot_of(direction, d - 1), rows], tok.at[slot_of(direction, d), rows],
                      first_send.at[direction, d - 1, q], first_recv.at[direction, d - 1, q], towards[direction])

    def second_copy(direction, d, q):
        rows = pl.ds((half_tok if direction == 0 else 0) + q * second_rows, second_rows)
        return remote(tok.at[slot_of(direction, d - 1), rows], tok.at[slot_of(direction, d), rows],
                      second_send.at[direction, d - 1, q], second_recv.at[direction, d - 1, q], towards[direction])

    def meta_copy(direction, d):
        return remote(meta.at[slot_of(direction, d - 1)], meta.at[slot_of(direction, d)],
                      meta_send.at[direction, d - 1], meta_recv.at[direction, d - 1], towards[direction])

    def meta_hops(direction):
        return far if direction == 0 else far - 1

    with scope('load'):
        load_tok.wait()
    with scope('barrier'):
        pl.semaphore_wait(barrier, 3)
    for q in range(firsts):
        for direction in both:
            first_copy(direction, 1, q).start()
            if q == 0:
                meta_copy(direction, 1).start()
    start_ab(0, 0)
    start_ab(1, 0)
    w2_copy(0, 0).start()
    w2_copy(1, 1).start()
    for d in range(1, far):
        with scope('ag_hop'):
            for q in range(firsts):
                for direction in both:
                    first_copy(direction, d, q).wait_recv()
                    first_copy(direction, d + 1, q).start()
                    if q == 0:
                        meta_copy(direction, d).wait_recv()
                        if d + 1 <= meta_hops(direction):
                            meta_copy(direction, d + 1).start()
    for q in range(seconds):
        for direction in both:
            second_copy(direction, 1, q).start()
    with scope('ag_far'):
        meta_copy(0, far).wait_recv()
        for q in range(firsts):
            for direction in both:
                first_copy(direction, far, q).wait_recv()

    def second_step(d, q):
        with scope('second_step'):
            for direction in both:
                second_copy(direction, d, q).wait_recv()
                if d + 1 < far:
                    second_copy(direction, d + 1, q).start()

    my_base = (z * chip_rows).astype(F32)
    my_core = (core * core_rows).astype(F32)

    def relative(slot):
        code = meta[slot, 0:top_k, :]
        rel = code - my_base
        inside = (code >= 0.0) & (rel >= 0.0) & (rel < float(chip_rows))
        rel = rel - my_core
        rel = jnp.where(rel < 0.0, rel + float(chip_rows), rel)
        return jnp.where(inside, rel, -1.0)

    def position():
        return lax.broadcasted_iota(jnp.int32, (chip_rows, tokens), 0).astype(F32)

    def select(i, slot):
        rel = relative(slot)
        pos = position()
        sel = jnp.zeros((chip_rows, tokens), F32)
        for k in range(top_k):
            sel = jnp.where(pos == rel[k:k + 1, :], 1.0, sel)
        sels[i] = sel.astype(BF16)

    def gather(i, slot):
        for n0, nw in chunks(hidden, 512):
            rows = jnp.dot(sels[i], tok[slot, :, n0:n0 + nw], preferred_element_type=F32).astype(BF16)
            xbuf[i, :, n0:n0 + nw] = rows[:core_rows]
            xsend[i, :, n0:n0 + nw] = rows[core_rows:]

    def weigh(i, slot):
        rel = relative(slot)
        gates = meta[slot, 8:8 + top_k, :]
        pos = position()
        w = jnp.zeros((chip_rows, tokens), F32)
        for k in range(top_k):
            w = jnp.where(pos == rel[k:k + 1, :], gates[k:k + 1, :], w)
        w = w.T
        hi = w.astype(BF16)
        rest = w - hi.astype(F32)
        mid = rest.astype(BF16)
        terms[i, 0] = hi
        terms[i, 1] = mid
        terms[i, 2] = (rest - mid.astype(F32)).astype(BF16)

    def combine(i, dst, p):
        for n0, nw in chunks(width, 256):
            cols = pl.ds(p * width + n0 if isinstance(p, int) else pl.multiple_of(p * width + n0, 128), nw)
            res = jnp.concatenate([rbuf[i, :, cols], rrecv[i, :, cols]], axis=0)
            acc = jnp.dot(terms[i, 0], res, preferred_element_type=F32)
            for t in (1, 2):
                acc = acc + jnp.dot(terms[i, t], res, preferred_element_type=F32)
            dst[:, cols] = acc

    def combine_all(*targets):
        def body(p, carry):
            for i, dst in targets:
                combine(i, dst, p)
            return carry

        with scope('combine'):
            lax.fori_loop(0, pieces, body, 0)

    def up_part(x_of, rows, which):
        lo, span = (0, ff_a) if which == 0 else (ff_a, ff_b)
        m1, m3 = (w1a, w3a) if which == 0 else (w1b, w3b)
        x = x_of()
        for n0, nw in chunks(span, 256):
            a = jnp.dot(x, m1[:, n0:n0 + nw], preferred_element_type=F32)
            b = jnp.dot(x, m3[:, n0:n0 + nw], preferred_element_type=F32)
            hbuf[0:rows, lo + n0:lo + n0 + nw] = (jax.nn.silu(a) * b).astype(BF16)

    def x_copy(phase, i, e):
        rows = pl.ds(pl.multiple_of(e * capacity, 16), capacity)
        return remote(xsend.at[i, rows], xbuf.at[2 + i, rows], x_send.at[phase, i, e], x_recv.at[phase, i, e], partner)

    def r_copy(phase, e):
        rows = pl.ds(pl.multiple_of(e * capacity, 16), capacity)
        return remote(rbuf.at[pl.ds(2, 2), rows], rrecv.at[:, rows], r_send.at[phase, e], r_recv.at[phase, e], partner)

    def expert_loop(phase, last, extra):
        def body(e, carry):
            row0 = pl.multiple_of(e * capacity, 16)
            nxt = (e + 1) % experts
            with scope('x_wait'):
                for i in both:
                    x_copy(phase, i, e).wait_recv()

            @pl.when(e < experts - 1)
            def _():
                for i in both:
                    x_copy(phase, i, e + 1).start()

            def x_of():
                return jnp.concatenate([xbuf[s, pl.ds(row0, capacity), :] for s in range(4)], axis=0)

            for which in both:
                with scope('wait_ab'):
                    wait_ab(which)
                with scope('up'):
                    up_part(x_of, 4 * capacity, which)
                if last:
                    @pl.when(e < experts - 1)
                    def _():
                        start_ab(which, nxt)

                    @pl.when(e == experts - 1)
                    def _():
                        start_shared_ab(which, 0)
                else:
                    start_ab(which, nxt)
                if extra is not None:
                    extra(e, which)
            if last:
                @pl.when((e >= 1) & (e < experts - 1))
                def _():
                    w2_copy(nxt, nxt % 2).start()

                @pl.when(e == experts - 1)
                def _():
                    shared_w2_copy(0, 0).start()
            else:
                @pl.when(e >= 1)
                def _():
                    w2_copy(nxt, nxt % 2).start()
            slot = e % 2
            with scope('wait_w2'):
                w2_copy(0, slot).wait()
            with scope('down'):
                for n0, nw in chunks(hidden, 256):
                    r = jnp.dot(hbuf[0:4 * capacity, :], w2s[slot, :, n0:n0 + nw], preferred_element_type=F32).astype(BF16)
                    for s in range(4):
                        rbuf[s, pl.ds(row0, capacity), n0:n0 + nw] = r[s * capacity:(s + 1) * capacity]
            r_copy(phase, e).start()

            @pl.when(e == experts - 1)
            def _():
                if last:
                    shared_w2_copy(1, 1).start()
                else:
                    w2_copy(1, 1).start()

            if extra is not None:
                extra(e, 2)
            return carry

        with scope('experts'):
            lax.fori_loop(0, experts, body, 0)

    def run_experts(phase, slots, last=False, extra=None, prepared=False):
        with scope('gather'):
            for i in both:
                if not prepared:
                    select(i, slots[i])
                gather(i, slots[i])
                x_copy(phase, i, 0).start()
        expert_loop(phase, last, extra)
        with scope('weigh'):
            for i in both:
                if not prepared:
                    weigh(i, slots[i])
        with scope('r_swap'):
            for e in range(experts):
                for i in both:
                    x_copy(phase, i, e).wait_send()
                r_copy(phase, e).wait()

    def rs_copy(direction, hop, p):
        cols = pl.ds(p * width if isinstance(p, int) else pl.multiple_of(p * width, 128), width)
        src = part.at[0, 0, :, cols] if hop == 1 else part.at[(hop - 1) % 2, direction, :, cols]
        return remote(src, rs.at[direction, (hop - 1) % 2, :, cols],
                      rs_send.at[direction, hop - 1, p], rs_recv.at[direction, hop - 1, p], towards[direction])

    def first_pieces(direction):
        half = pieces // 2
        return range(0, half) if direction == 0 else range(half, pieces)

    def order(direction, j):
        return (j + pieces // 2) % pieces if direction == 0 else j

    def forward(direction, hop, p, add):
        if add:
            rs_copy(direction, hop - 1, p).wait_recv()
            cols = pl.ds(p * width if isinstance(p, int) else pl.multiple_of(p * width, 128), width)
            mine = part.at[(hop - 1) % 2, direction, :, cols]
            mine[...] = mine[...] + rs[direction, hop % 2, :, cols]
        rs_copy(direction, hop, p).start()

    def give_credit(which):
        for direction in both:
            pl.semaphore_signal(credit.at[direction, which], inc=1, device_id={'ep': origin[direction]}, device_id_type=MESH)

    def take_credit(which):
        for direction in both:
            pl.semaphore_wait(credit.at[direction, which], 1)

    def wait_sends(hop):
        with scope('wait_sends'):
            for direction in both:
                for p in (first_pieces(direction) if hop == 1 else range(pieces)):
                    rs_copy(direction, hop, p).wait_send()

    def pair(d):
        return [slot_of(1, d), slot_of(0, d)]

    points = ((1, 0), (2, 1), (3, 2))

    def gather_service(e, stage):
        for n, (at_e, at_stage) in enumerate(points):
            if stage == at_stage:
                @pl.when(e == at_e)
                def _():
                    second_step(1 + n // seconds, n % seconds)

    run_experts(0, [slot_of(0, far), 0], extra=gather_service)
    steps = [(d, q) for d in range(1, far) for q in range(seconds)]
    before = (far - 2) * seconds
    combine_all((0, part.at[0, 0]))
    for d, q in steps[len(points):before]:
        second_step(d, q)
    for j in range(pieces // 2):
        for direction in both:
            rs_copy(direction, 1, first_pieces(direction)[j]).start()
    combine_all((1, base))
    for i in both:
        select(i, pair(far - 1)[i])
        weigh(i, pair(far - 1)[i])
    for d, q in steps[before:]:
        second_step(d, q)

    run_experts(1, pair(far - 1), prepared=True)
    with scope('combine'):
        for j in range(pieces):
            for direction in both:
                p = order(direction, j)
                combine(direction, part.at[1, direction], p)
                forward(direction, 2, p, p in first_pieces(direction))
    give_credit(0)

    run_experts(2, pair(far - 2))
    wait_sends(1)
    combine_all((0, part.at[0, 0]), (1, part.at[0, 1]))
    take_credit(0)

    def service(e, stage):
        if stage == 2:
            with scope('extra'):
                for direction in both:
                    forward(direction, 3, order(direction, e), True)

    run_experts(3, pair(far - 3), last=True, extra=service)
    give_credit(1)
    wait_sends(2)
    combine_all((0, part.at[1, 0]), (1, part.at[1, 1]))

    products = jnp.zeros((tokens, 128), F32)
    for j in range(hidden // 128):
        products = products + tok[0, :, j * 128:(j + 1) * 128].astype(F32) * gate_ref[j:j + 1, :].astype(F32)
    scale = jax.nn.sigmoid(jnp.sum(products, axis=1, keepdims=True))

    def shared_body(i, carry):
        for which in both:
            wait_ab(which)
            up_part(lambda: tok[0], tokens, which)

            @pl.when(i == 0)
            def _():
                start_shared_ab(which, 1)
        w2_copy(0, i).wait()
        for n0, nw in chunks(hidden, 256):
            s = jnp.dot(hbuf[0:tokens, :], w2s[i, :, n0:n0 + nw], preferred_element_type=F32)
            base[:, n0:n0 + nw] = base[:, n0:n0 + nw] + scale * s
        return carry

    with scope('shared'):
        lax.fori_loop(0, 2, shared_body, 0)

    take_credit(1)
    with scope('last_hop'):
        for j in range(pieces):
            for direction in both:
                forward(direction, far, order(direction, j), True)

    with scope('finish'):
        half = pieces // 2
        for j in range(half):
            for p in (j, j + half):
                cols = pl.ds(p * width, width)
                total = tok[0, :, cols].astype(F32) + base[:, cols]
                for direction in both:
                    rs_copy(direction, far, p).wait_recv()
                    total = total + rs[direction, (far - 1) % 2, :, cols]
                y[:, cols] = total.astype(BF16)
                pltpu.make_async_copy(y.at[:, cols], out_ref.at[:, cols], out_sem.at[p]).start()

    for direction in both:
        for d in range(1, far + 1):
            for q in range(firsts):
                first_copy(direction, d, q).wait_send()
            if d < far:
                for q in range(seconds):
                    second_copy(direction, d, q).wait_send()
            if d <= meta_hops(direction):
                meta_copy(direction, d).wait_send()
    wait_sends(3)
    wait_sends(4)
    with scope('out'):
        for p in range(pieces):
            cols = pl.ds(p * width, width)
            pltpu.make_async_copy(y.at[:, cols], out_ref.at[:, cols], out_sem.at[p]).wait()


def solution(mesh):
    num_ep = mesh.shape['ep']
    row_spec = P(('dp', 'ep'), None)
    replicated = P()
    expert_spec = P('ep', None, None)

    def device_step(tokens, expert_ids, gate_vals, slots, shared_w1, shared_w3, shared_w2, shared_gate, expert_w1, expert_w3, expert_w2):
        tok_count, hidden = tokens.shape
        top_k = expert_ids.shape[1]
        experts, _, ff = expert_w1.shape
        num_experts = experts * num_ep
        capacity = 8 * ((2 * tok_count * top_k + 8 * num_experts - 1) // (8 * num_experts))
        core_rows = experts * capacity
        far = num_ep // 4
        ff_a = 256 * ((ff + 511) // 512)
        ff_b = ff - ff_a

        vmem = pl.BlockSpec(memory_space=pltpu.VMEM)
        hbm = pl.BlockSpec(memory_space=pl.ANY)
        dma = pltpu.SemaphoreType.DMA
        return pl.pallas_call(
            functools.partial(moe_kernel, num_ep, capacity),
            out_shape=jax.ShapeDtypeStruct((tok_count, hidden), BF16),
            in_specs=[hbm, vmem, vmem, vmem, vmem] + [hbm] * 6,
            out_specs=hbm,
            scratch_shapes=[
                pltpu.VMEM((2 * far, tok_count, hidden), BF16),
                pltpu.VMEM((2 * far, 16, tok_count), F32),
                pltpu.VMEM((hidden, ff_a), BF16),
                pltpu.VMEM((hidden, ff_b), BF16),
                pltpu.VMEM((hidden, ff_a), BF16),
                pltpu.VMEM((hidden, ff_b), BF16),
                pltpu.VMEM((2, ff, hidden), BF16),
                pltpu.VMEM((4, core_rows, hidden), BF16),
                pltpu.VMEM((2, core_rows, hidden), BF16),
                pltpu.VMEM((4, core_rows, hidden), BF16),
                pltpu.VMEM((2, core_rows, hidden), BF16),
                pltpu.VMEM((tok_count, ff), BF16),
                pltpu.VMEM((2, 2, tok_count, hidden), F32),
                pltpu.VMEM((2, 2, tok_count, hidden), F32),
                pltpu.VMEM((tok_count, hidden), F32),
                pltpu.VMEM((2, 2 * core_rows, tok_count), BF16),
                pltpu.VMEM((2, 3, tok_count, 2 * core_rows), BF16),
                pltpu.VMEM((tok_count, hidden), BF16),
                dma((1,)), dma((4,)), dma((2, 2)), dma((2,)),
                dma((2, far, 4)), dma((2, far, 4)), dma((2, far - 1, 2)), dma((2, far - 1, 2)), dma((2, far)), dma((2, far)),
                dma((far, 2, experts)), dma((far, 2, experts)), dma((far, experts)), dma((far, experts)),
                dma((2, far, 4)), dma((2, far, 4)), pltpu.SemaphoreType.REGULAR((2, 2)),
            ],
            compiler_params=pltpu.CompilerParams(collective_id=0, has_side_effects=True, vmem_limit_bytes=66_000_000),
        )(tokens, expert_ids.T, slots.T, gate_vals.T, shared_gate.reshape(hidden // 128, 128), shared_w1, shared_w3, shared_w2, expert_w1, expert_w3, expert_w2)

    return jax.shard_map(device_step, mesh=mesh, in_specs=(row_spec, row_spec, row_spec, row_spec, replicated, replicated, replicated, replicated, expert_spec, expert_spec, expert_spec), out_specs=row_spec, check_vma=False)
```

```python
import functools

import jax
import jax.numpy as jnp
from jax import lax
from jax.experimental import pallas as pl
from jax.experimental.pallas import tpu as pltpu
from jax.sharding import PartitionSpec as P

MESH = pl.DeviceIdType.MESH
F32 = jnp.float32
BF16 = jnp.bfloat16


def chunks(total, width):
    return [(start, min(width, total - start)) for start in range(0, total, width)]


def moe_kernel(num_ep, capacity,
               tok_hbm, ids_ref, slots_ref, gates_ref, gate_ref, ws1, ws3, ws2, we1, we3, we2,
               out_ref,
               tok, meta, w1a, w1b, w3a, w3b, w2s, xbuf, xsend, rbuf, rrecv, hbuf, part, rs, base, sels, terms, y,
               load_sem, out_sem, ab_sem, w2_sem,
               first_send, first_recv, second_send, second_recv, meta_send, meta_recv,
               x_send, x_recv, r_send, r_recv, rs_send, rs_recv, credit):
    scope = jax.named_scope
    tokens, hidden = tok.shape[1:]
    top_k = ids_ref.shape[0]
    experts = we1.shape[0]
    ff = we1.shape[2]
    ff_a, ff_b = w1a.shape[1], w1b.shape[1]
    half_tok = tokens // 2
    nz = num_ep // 2
    far = nz // 2
    core_rows = experts * capacity
    chip_rows = 2 * core_rows
    pieces = rs_send.shape[2]
    width = hidden // pieces
    firsts = first_send.shape[2]
    first_rows = half_tok // firsts
    seconds = second_send.shape[2]
    second_rows = half_tok // seconds

    ep = lax.axis_index('ep')
    z, core = ep // 2, ep % 2
    right = (ep + 2) % num_ep
    left = (ep + num_ep - 2) % num_ep
    partner = z * 2 + 1 - core
    towards = (right, left)
    origin = (left, right)
    both = (0, 1)

    barrier = pltpu.get_barrier_semaphore()
    for other in (left, right, partner):
        pl.semaphore_signal(barrier, inc=1, device_id={'ep': other}, device_id_type=MESH)

    load_tok = pltpu.make_async_copy(tok_hbm, tok.at[0], load_sem.at[0])
    load_tok.start()
    meta[0, 0:top_k, :] = jnp.where(slots_ref[...] >= 0, ids_ref[...] * capacity + slots_ref[...], -1).astype(F32)
    meta[0, 8:8 + top_k, :] = gates_ref[...]

    def ab_copies(which, m1, m3, lead, col):
        lo, span = (0, ff_a) if which == 0 else (ff_a, ff_b)
        dst1, dst3 = (w1a, w3a) if which == 0 else (w1b, w3b)
        cols = pl.ds(col + lo, span)
        src1 = m1.at[lead, :, cols] if lead is not None else m1.at[:, cols]
        src3 = m3.at[lead, :, cols] if lead is not None else m3.at[:, cols]
        return (pltpu.make_async_copy(src1, dst1, ab_sem.at[which, 0]),
                pltpu.make_async_copy(src3, dst3, ab_sem.at[which, 1]))

    def start_ab(which, e):
        for c in ab_copies(which, we1, we3, e, 0):
            c.start()

    def start_shared_ab(which, i):
        for c in ab_copies(which, ws1, ws3, None, i * ff):
            c.start()

    def wait_ab(which):
        for c in ab_copies(which, we1, we3, 0, 0):
            c.wait()

    def w2_copy(e, slot):
        return pltpu.make_async_copy(we2.at[e], w2s.at[slot], w2_sem.at[slot])

    def shared_w2_copy(i, slot):
        return pltpu.make_async_copy(ws2.at[pl.ds(i * ff, ff)], w2s.at[slot], w2_sem.at[slot])

    def slot_of(direction, d):
        if d == 0:
            return 0
        if d == far:
            return 2 * far - 1
        return d if direction == 0 else far - 1 + d

    def remote(src, dst, send_sem, recv_sem, device):
        return pltpu.make_async_remote_copy(src_ref=src, dst_ref=dst, send_sem=send_sem, recv_sem=recv_sem,
                                            device_id={'ep': device}, device_id_type=MESH)

    def first_copy(direction, d, q):
        rows = pl.ds((0 if direction == 0 else half_tok) + q * first_rows, first_rows)
        return remote(tok.at[slot_of(direction, d - 1), rows], tok.at[slot_of(direction, d), rows],
                      first_send.at[direction, d - 1, q], first_recv.at[direction, d - 1, q], towards[direction])

    def second_copy(direction, d, q):
        rows = pl.ds((half_tok if direction == 0 else 0) + q * second_rows, second_rows)
        return remote(tok.at[slot_of(direction, d - 1), rows], tok.at[slot_of(direction, d), rows],
                      second_send.at[direction, d - 1, q], second_recv.at[direction, d - 1, q], towards[direction])

    def meta_copy(direction, d):
        return remote(meta.at[slot_of(direction, d - 1)], meta.at[slot_of(direction, d)],
                      meta_send.at[direction, d - 1], meta_recv.at[direction, d - 1], towards[direction])

    def meta_hops(direction):
        return far if direction == 0 else far - 1

    with scope('load'):
        load_tok.wait()
    with scope('barrier'):
        pl.semaphore_wait(barrier, 3)
    for q in range(firsts):
        for direction in both:
            first_copy(direction, 1, q).start()
            if q == 0:
                meta_copy(direction, 1).start()
    start_ab(0, 0)
    start_ab(1, 0)
    w2_copy(0, 0).start()
    w2_copy(1, 1).start()
    for d in range(1, far):
        with scope('ag_hop'):
            for q in range(firsts):
                for direction in both:
                    first_copy(direction, d, q).wait_recv()
                    first_copy(direction, d + 1, q).start()
                    if q == 0:
                        meta_copy(direction, d).wait_recv()
                        if d + 1 <= meta_hops(direction):
                            meta_copy(direction, d + 1).start()
    for q in range(seconds):
        for direction in both:
            second_copy(direction, 1, q).start()
    with scope('ag_far'):
        meta_copy(0, far).wait_recv()
        for q in range(firsts):
            for direction in both:
                first_copy(direction, far, q).wait_recv()

    def second_step(d, q):
        with scope('second_step'):
            for direction in both:
                second_copy(direction, d, q).wait_recv()
                if d + 1 < far:
                    second_copy(direction, d + 1, q).start()

    my_base = (z * chip_rows).astype(F32)
    my_core = (core * core_rows).astype(F32)

    def relative(slot):
        code = meta[slot, 0:top_k, :]
        rel = code - my_base
        inside = (code >= 0.0) & (rel >= 0.0) & (rel < float(chip_rows))
        rel = rel - my_core
        rel = jnp.where(rel < 0.0, rel + float(chip_rows), rel)
        return jnp.where(inside, rel, -1.0)

    def position():
        return lax.broadcasted_iota(jnp.int32, (chip_rows, tokens), 0).astype(F32)

    def select(i, slot):
        rel = relative(slot)
        pos = position()
        sel = jnp.zeros((chip_rows, tokens), F32)
        for k in range(top_k):
            sel = jnp.where(pos == rel[k:k + 1, :], 1.0, sel)
        sels[i] = sel.astype(BF16)

    def gather(i, slot):
        for n0, nw in chunks(hidden, 512):
            rows = jnp.dot(sels[i], tok[slot, :, n0:n0 + nw], preferred_element_type=F32).astype(BF16)
            xbuf[i, :, n0:n0 + nw] = rows[:core_rows]
            xsend[i, :, n0:n0 + nw] = rows[core_rows:]

    def weigh(i, slot):
        rel = relative(slot)
        gates = meta[slot, 8:8 + top_k, :]
        pos = position()
        w = jnp.zeros((chip_rows, tokens), F32)
        for k in range(top_k):
            w = jnp.where(pos == rel[k:k + 1, :], gates[k:k + 1, :], w)
        w = w.T
        hi = w.astype(BF16)
        rest = w - hi.astype(F32)
        mid = rest.astype(BF16)
        terms[i, 0] = hi
        terms[i, 1] = mid
        terms[i, 2] = (rest - mid.astype(F32)).astype(BF16)

    def combine(i, dst, p):
        for n0, nw in chunks(width, 256):
            cols = pl.ds(p * width + n0 if isinstance(p, int) else pl.multiple_of(p * width + n0, 128), nw)
            res = jnp.concatenate([rbuf[i, :, cols], rrecv[i, :, cols]], axis=0)
            acc = jnp.dot(terms[i, 0], res, preferred_element_type=F32)
            for t in (1, 2):
                acc = acc + jnp.dot(terms[i, t], res, preferred_element_type=F32)
            dst[:, cols] = acc

    def combine_all(*targets):
        def body(p, carry):
            for i, dst in targets:
                combine(i, dst, p)
            return carry

        with scope('combine'):
            lax.fori_loop(0, pieces, body, 0)

    def up_part(x_of, rows, which):
        lo, span = (0, ff_a) if which == 0 else (ff_a, ff_b)
        m1, m3 = (w1a, w3a) if which == 0 else (w1b, w3b)
        x = x_of()
        for n0, nw in chunks(span, 256):
            a = jnp.dot(x, m1[:, n0:n0 + nw], preferred_element_type=F32)
            b = jnp.dot(x, m3[:, n0:n0 + nw], preferred_element_type=F32)
            hbuf[0:rows, lo + n0:lo + n0 + nw] = (jax.nn.silu(a) * b).astype(BF16)

    def x_copy(i, e):
        rows = pl.ds(pl.multiple_of(e * capacity, 16), capacity)
        return remote(xsend.at[i, rows], xbuf.at[2 + i, rows], x_send.at[i, e], x_recv.at[i, e], partner)

    def r_copy(e):
        rows = pl.ds(pl.multiple_of(e * capacity, 16), capacity)
        return remote(rbuf.at[pl.ds(2, 2), rows], rrecv.at[:, rows], r_send.at[e], r_recv.at[e], partner)

    def expert_loop(phase, last, extra):
        def body(e, carry):
            row0 = pl.multiple_of(e * capacity, 16)
            nxt = (e + 1) % experts
            with scope('x_wait'):
                for i in both:
                    x_copy(i, e).wait_recv()

            @pl.when(e < experts - 1)
            def _():
                for i in both:
                    x_copy(i, e + 1).start()

            def x_of():
                return jnp.concatenate([xbuf[s, pl.ds(row0, capacity), :] for s in range(4)], axis=0)

            for which in both:
                with scope('wait_ab'):
                    wait_ab(which)
                with scope('up'):
                    up_part(x_of, 4 * capacity, which)
                if last:
                    @pl.when(e < experts - 1)
                    def _():
                        start_ab(which, nxt)

                    @pl.when(e == experts - 1)
                    def _():
                        start_shared_ab(which, 0)
                else:
                    start_ab(which, nxt)
                if extra is not None:
                    extra(e, which)
            if last:
                @pl.when((e >= 1) & (e < experts - 1))
                def _():
                    w2_copy(nxt, nxt % 2).start()

                @pl.when(e == experts - 1)
                def _():
                    shared_w2_copy(0, 0).start()
            else:
                @pl.when(e >= 1)
                def _():
                    w2_copy(nxt, nxt % 2).start()
            slot = e % 2
            with scope('wait_w2'):
                w2_copy(0, slot).wait()
            with scope('down'):
                for n0, nw in chunks(hidden, 256):
                    r = jnp.dot(hbuf[0:4 * capacity, :], w2s[slot, :, n0:n0 + nw], preferred_element_type=F32).astype(BF16)
                    for s in range(4):
                        rbuf[s, pl.ds(row0, capacity), n0:n0 + nw] = r[s * capacity:(s + 1) * capacity]
            r_copy(e).start()

            @pl.when(e == experts - 1)
            def _():
                if last:
                    shared_w2_copy(1, 1).start()
                else:
                    w2_copy(1, 1).start()

            if extra is not None:
                extra(e, 2)
            return carry

        with scope('experts'):
            lax.fori_loop(0, experts, body, 0)

    def run_experts(phase, slots, last=False, extra=None, prepared=False):
        with scope('gather'):
            for i in both:
                if not prepared:
                    select(i, slots[i])
                gather(i, slots[i])
                x_copy(i, 0).start()
        expert_loop(phase, last, extra)
        with scope('weigh'):
            for i in both:
                if not prepared:
                    weigh(i, slots[i])
        with scope('r_swap'):
            for e in range(experts):
                for i in both:
                    x_copy(i, e).wait_send()
                r_copy(e).wait()

    def rs_copy(direction, hop, p):
        cols = pl.ds(p * width if isinstance(p, int) else pl.multiple_of(p * width, 128), width)
        src = part.at[0, 0, :, cols] if hop == 1 else part.at[(hop - 1) % 2, direction, :, cols]
        return remote(src, rs.at[direction, (hop - 1) % 2, :, cols],
                      rs_send.at[direction, (hop - 1) % 2, p], rs_recv.at[direction, (hop - 1) % 2, p], towards[direction])

    def first_pieces(direction):
        half = pieces // 2
        return range(0, half) if direction == 0 else range(half, pieces)

    def order(direction, j):
        return (j + pieces // 2) % pieces if direction == 0 else j

    def forward(direction, hop, p, add):
        if add:
            rs_copy(direction, hop - 1, p).wait_recv()
            cols = pl.ds(p * width if isinstance(p, int) else pl.multiple_of(p * width, 128), width)
            mine = part.at[(hop - 1) % 2, direction, :, cols]
            mine[...] = mine[...] + rs[direction, hop % 2, :, cols]
        rs_copy(direction, hop, p).start()

    def give_credit(which):
        for direction in both:
            pl.semaphore_signal(credit.at[direction, which], inc=1, device_id={'ep': origin[direction]}, device_id_type=MESH)

    def take_credit(which):
        for direction in both:
            pl.semaphore_wait(credit.at[direction, which], 1)

    def wait_sends(hop):
        with scope('wait_sends'):
            for direction in both:
                for p in (first_pieces(direction) if hop == 1 else range(pieces)):
                    rs_copy(direction, hop, p).wait_send()

    def pair(d):
        return [slot_of(1, d), slot_of(0, d)]

    points = ((1, 0), (2, 1), (3, 2))

    def gather_service(e, stage):
        for n, (at_e, at_stage) in enumerate(points):
            if stage == at_stage:
                @pl.when(e == at_e)
                def _():
                    second_step(1 + n // seconds, n % seconds)

    run_experts(0, [slot_of(0, far), 0], extra=gather_service)
    steps = [(d, q) for d in range(1, far) for q in range(seconds)]
    before = (far - 2) * seconds
    combine_all((0, part.at[0, 0]))
    for d, q in steps[len(points):before]:
        second_step(d, q)
    for j in range(pieces // 2):
        for direction in both:
            rs_copy(direction, 1, first_pieces(direction)[j]).start()
    combine_all((1, base))
    for i in both:
        select(i, pair(far - 1)[i])
        weigh(i, pair(far - 1)[i])
    for d, q in steps[before:]:
        second_step(d, q)

    run_experts(1, pair(far - 1), prepared=True)
    with scope('combine'):
        for j in range(pieces):
            for direction in both:
                p = order(direction, j)
                combine(direction, part.at[1, direction], p)
                forward(direction, 2, p, p in first_pieces(direction))
    give_credit(0)

    run_experts(2, pair(far - 2))
    wait_sends(1)
    combine_all((0, part.at[0, 0]), (1, part.at[0, 1]))
    take_credit(0)

    def service(e, stage):
        if stage == 2:
            with scope('extra'):
                for direction in both:
                    forward(direction, 3, order(direction, e), True)

    run_experts(3, pair(far - 3), last=True, extra=service)
    give_credit(1)
    wait_sends(2)
    combine_all((0, part.at[1, 0]), (1, part.at[1, 1]))

    products = jnp.zeros((tokens, 128), F32)
    for j in range(hidden // 128):
        products = products + tok[0, :, j * 128:(j + 1) * 128].astype(F32) * gate_ref[j:j + 1, :].astype(F32)
    scale = jax.nn.sigmoid(jnp.sum(products, axis=1, keepdims=True))

    def shared_body(i, carry):
        for which in both:
            wait_ab(which)
            up_part(lambda: tok[0], tokens, which)

            @pl.when(i == 0)
            def _():
                start_shared_ab(which, 1)
        w2_copy(0, i).wait()
        for n0, nw in chunks(hidden, 256):
            s = jnp.dot(hbuf[0:tokens, :], w2s[i, :, n0:n0 + nw], preferred_element_type=F32)
            base[:, n0:n0 + nw] = base[:, n0:n0 + nw] + scale * s
        return carry

    with scope('shared'):
        lax.fori_loop(0, 2, shared_body, 0)

    take_credit(1)
    with scope('last_hop'):
        for j in range(pieces):
            for direction in both:
                forward(direction, far, order(direction, j), True)

    with scope('finish'):
        half = pieces // 2
        for j in range(half):
            for p in (j, j + half):
                cols = pl.ds(p * width, width)
                total = tok[0, :, cols].astype(F32) + base[:, cols]
                for direction in both:
                    rs_copy(direction, far, p).wait_recv()
                    total = total + rs[direction, (far - 1) % 2, :, cols]
                y[:, cols] = total.astype(BF16)
                pltpu.make_async_copy(y.at[:, cols], out_ref.at[:, cols], out_sem.at[p]).start()

    for direction in both:
        for d in range(1, far + 1):
            for q in range(firsts):
                first_copy(direction, d, q).wait_send()
            if d < far:
                for q in range(seconds):
                    second_copy(direction, d, q).wait_send()
            if d <= meta_hops(direction):
                meta_copy(direction, d).wait_send()
    wait_sends(3)
    wait_sends(4)
    with scope('out'):
        for p in range(pieces):
            cols = pl.ds(p * width, width)
            pltpu.make_async_copy(y.at[:, cols], out_ref.at[:, cols], out_sem.at[p]).wait()


def solution(mesh):
    num_ep = mesh.shape['ep']
    row_spec = P(('dp', 'ep'), None)
    replicated = P()
    expert_spec = P('ep', None, None)

    def device_step(tokens, expert_ids, gate_vals, slots, shared_w1, shared_w3, shared_w2, shared_gate, expert_w1, expert_w3, expert_w2):
        tok_count, hidden = tokens.shape
        top_k = expert_ids.shape[1]
        experts, _, ff = expert_w1.shape
        num_experts = experts * num_ep
        capacity = 8 * ((2 * tok_count * top_k + 8 * num_experts - 1) // (8 * num_experts))
        core_rows = experts * capacity
        far = num_ep // 4
        ff_a = 256 * ((ff + 511) // 512)
        ff_b = ff - ff_a

        vmem = pl.BlockSpec(memory_space=pltpu.VMEM)
        hbm = pl.BlockSpec(memory_space=pl.ANY)
        dma = pltpu.SemaphoreType.DMA
        return pl.pallas_call(
            functools.partial(moe_kernel, num_ep, capacity),
            out_shape=jax.ShapeDtypeStruct((tok_count, hidden), BF16),
            in_specs=[hbm, vmem, vmem, vmem, vmem] + [hbm] * 6,
            out_specs=hbm,
            scratch_shapes=[
                pltpu.VMEM((2 * far, tok_count, hidden), BF16),
                pltpu.VMEM((2 * far, 16, tok_count), F32),
                pltpu.VMEM((hidden, ff_a), BF16),
                pltpu.VMEM((hidden, ff_b), BF16),
                pltpu.VMEM((hidden, ff_a), BF16),
                pltpu.VMEM((hidden, ff_b), BF16),
                pltpu.VMEM((2, ff, hidden), BF16),
                pltpu.VMEM((4, core_rows, hidden), BF16),
                pltpu.VMEM((2, core_rows, hidden), BF16),
                pltpu.VMEM((4, core_rows, hidden), BF16),
                pltpu.VMEM((2, core_rows, hidden), BF16),
                pltpu.VMEM((tok_count, ff), BF16),
                pltpu.VMEM((2, 2, tok_count, hidden), F32),
                pltpu.VMEM((2, 2, tok_count, hidden), F32),
                pltpu.VMEM((tok_count, hidden), F32),
                pltpu.VMEM((2, 2 * core_rows, tok_count), BF16),
                pltpu.VMEM((2, 3, tok_count, 2 * core_rows), BF16),
                pltpu.VMEM((tok_count, hidden), BF16),
                dma((1,)), dma((4,)), dma((2, 2)), dma((2,)),
                dma((2, far, 4)), dma((2, far, 4)), dma((2, far - 1, 2)), dma((2, far - 1, 2)), dma((2, far)), dma((2, far)),
                dma((2, experts)), dma((2, experts)), dma((experts,)), dma((experts,)),
                dma((2, 2, 4)), dma((2, 2, 4)), pltpu.SemaphoreType.REGULAR((2, 2)),
            ],
            compiler_params=pltpu.CompilerParams(collective_id=0, has_side_effects=True, vmem_limit_bytes=66_000_000),
        )(tokens, expert_ids.T, slots.T, gate_vals.T, shared_gate.reshape(hidden // 128, 128), shared_w1, shared_w3, shared_w2, expert_w1, expert_w3, expert_w2)

    return jax.shard_map(device_step, mesh=mesh, in_specs=(row_spec, row_spec, row_spec, row_spec, replicated, replicated, replicated, replicated, expert_spec, expert_spec, expert_spec), out_specs=row_spec, check_vma=False)
```
